32 devices in a mesh: wide: 8 (over z, core), narrow: 4 (over y, x).
Axes of the slice: x: 2, y: 2, z: 4, core: 2. Of those that a mesh axis runs over, the one named last changes fastest.
Arguments:
- tridiag_vectors: float32 [128, 131072], P(('wide', 'narrow')), may hold values from -6 to 6
- reflectors: float32 [2, 131072, 256], P(None, 'wide'), may hold values from -0.015625 to 0.015625
- triangles: float32 [2, 256, 256], replicated, as said below
- lower_blocks: float32 [6, 1536, 1536], P(None, 'wide'), may hold values from -0.109375 to 0.109375
- diag_inverses: float32 [4, 1536, 1536], P(None, None, 'wide'), as said below
Outputs:
- transformed: float32 [128, 131072], P('narrow', 'wide')
- solved: float32 [128, 4, 1536], P('narrow', None, 'wide')
The draws below stay inside these ranges and needn't reach their ends.
Inputs may be any that keep to these rules, and one draw needn't show every extreme that they name: `triangles`: zero below the diagonal, positive on it. `diag_inverses`: zero above the diagonal, positive on it.
All inputs are finite; a program needn't handle non-finite values.
Results may differ from the reference program's by a relative error of at most 0.00019.
Values sent between devices are 32-bit elements; how exact they have to be, the bound alone decides.
A program may use at most 128 MiB of HBM per device.

```python
import math
import jax
import jax.numpy as jnp
from jax import lax

N = 131072
K = 128
NB = 256
PANELS = 4
PANEL = 1536
BLOCKS = 6


def draw_triangles(key, part):
    key_diag, key_upper = jax.random.split(jax.random.fold_in(key, 11))
    factor = math.sqrt(N / NB)
    diagon = jnp.exp(jax.random.uniform(key_diag, (2, NB), jnp.float32, math.log(0.5), math.log(2.0)))
    upper = jax.random.truncated_normal(key_upper, -4.0, 4.0, (2, NB, NB), jnp.float32) / math.sqrt(NB)
    strict = jnp.triu(jnp.ones((NB, NB), jnp.float32), 1)
    return factor * (upper * strict + diagon[:, :, None] * jnp.eye(NB, dtype=jnp.float32))


def draw_diag_inverses(key, part):
    key_diag, key_lower = jax.random.split(jax.random.fold_in(key, 23))
    diagon = jnp.exp(jax.random.uniform(key_diag, (PANELS, PANEL), jnp.float32, math.log(0.5), math.log(2.0)))
    lower = 0.5 * jax.random.truncated_normal(key_lower, -4.0, 4.0, (PANELS, PANEL, PANEL), jnp.float32) / math.sqrt(PANEL)
    strict = jnp.tril(jnp.ones((PANEL, PANEL), jnp.float32), -1)
    return lower * strict + diagon[:, :, None] * jnp.eye(PANEL, dtype=jnp.float32)


def shard_levels(key, shape, pieces, smallest, high):
    loudness = 1.0
    for dim, shards_of in pieces:
        draws = jax.random.uniform(jax.random.fold_in(jax.random.fold_in(key, 6), dim), (shards_of,), jnp.float32, smallest / len(pieces), high / len(pieces))
        loudness = loudness * jnp.repeat(jnp.exp(draws), shape[dim] // shards_of).reshape((-1,) + (1,) * (len(shape) - 1 - dim))
    return loudness


def scatter_about(stream_key, dims, deviation, bound, shards=(), held_as=jnp.bfloat16):
    drawn = jax.random.normal(stream_key, dims, jnp.float32) * deviation
    if len(shards) > 0:
        drawn = shard_levels(stream_key, dims, shards, -0.22, 0.18) * drawn
    return jnp.clip(drawn, min=-bound, max=bound).astype(held_as)


def setup_inputs(seed: int = 0) -> dict:
    seeds = jax.random.split(jax.random.key(seed), 6)
    tridiag_vectors = scatter_about(seeds[0], (K, N), 1.0, 6.0, ((0, 32),), jnp.float32)
    reflectors = scatter_about(seeds[1], (2, N, NB), N ** -0.5, 0.015625, ((1, 8),), jnp.float32)
    triangles = draw_triangles(jax.random.fold_in(seeds[5], 71), 0)
    lower_blocks = scatter_about(seeds[3], (BLOCKS, PANEL, PANEL), (2 * PANEL) ** -0.5, 0.109375, ((1, 8),), jnp.float32)
    diag_inverses = draw_diag_inverses(jax.random.fold_in(seeds[5], 71), 0)
    return dict(tridiag_vectors=tridiag_vectors, reflectors=reflectors, triangles=triangles, lower_blocks=lower_blocks, diag_inverses=diag_inverses)


HIGHEST = lax.Precision.HIGHEST


def reference(tridiag_vectors, reflectors, triangles, lower_blocks, diag_inverses):
    current = tridiag_vectors
    for which in (1, 0):
        products = jnp.dot(current, reflectors[which], precision=HIGHEST)
        coeffs = jnp.dot(products, triangles[which].T, precision=HIGHEST)
        current = current - jnp.dot(coeffs, reflectors[which].T, precision=HIGHEST)
    corner = current[:, N - PANELS * PANEL:].reshape(K, PANELS, PANEL)
    results = [None] * PANELS
    for source in reversed(range(PANELS)):
        remain = corner[:, source, :]
        for higher in range(source + 1, PANELS):
            index_block = higher * (higher - 1) // 2 + source
            remain = remain - jnp.dot(results[higher], lower_blocks[index_block], precision=HIGHEST)
        results[source] = jnp.dot(remain, diag_inverses[source], precision=HIGHEST)
    return current, jnp.stack(results, axis=1)
```

```python
import functools

import jax
import jax.numpy as jnp
from jax import lax
from jax.experimental import pallas as pl
from jax.experimental.pallas import tpu as pltpu
from jax.sharding import PartitionSpec as P

HIGHEST = lax.Precision.HIGHEST
MESH = pl.DeviceIdType.MESH
ANY = pl.ANY
VMEM = pltpu.VMEM


def greet(axes):
    barrier = pltpu.get_barrier_semaphore()
    total = 0
    for axis, size in axes:
        here = lax.axis_index(axis)
        for k in range(1, size):
            pl.semaphore_signal(
                barrier, inc=1, device_id={axis: lax.rem(here + k, size)}, device_id_type=MESH
            )
        total += size - 1
    pl.semaphore_wait(barrier, total)


def remote(src, dst, send, recv, axis, target):
    return pltpu.make_async_remote_copy(
        src_ref=src, dst_ref=dst, send_sem=send, recv_sem=recv,
        device_id={axis: target}, device_id_type=MESH,
    )


def spread_kernel(wide, narrow, z_ref, buf_ref, bounce, send1, recv1, send2, recv2, local_sem):
    w = lax.axis_index("wide")
    n = lax.axis_index("narrow")
    cols = buf_ref.shape[2]

    def piece(target):
        return z_ref.at[:, pl.ds(pl.multiple_of(target * cols, 128), cols)]

    def owner(source):
        return (source * narrow + n) // wide

    def slot(source):
        return (source * narrow + n) % wide

    greet((("wide", wide), ("narrow", narrow)))
    place = jnp.where(owner(w) == n, slot(w), wide + w)
    for k in range(1, wide):
        target = lax.rem(w + k, wide)
        remote(piece(target), buf_ref.at[place], send1.at[k], recv1.at[w], "wide", target).start()

    mine = owner(w) == n

    @pl.when(mine)
    def _():
        first = pltpu.make_async_copy(piece(w), bounce, local_sem.at[0])
        first.start()
        first.wait()
        pltpu.make_async_copy(bounce, buf_ref.at[slot(w)], local_sem.at[1]).start()

    @pl.when(jnp.logical_not(mine))
    def _():
        s = slot(w)
        remote(piece(w), buf_ref.at[s], send2.at[w], recv2.at[s], "narrow", owner(w)).start()

    for k in range(1, wide):
        source = lax.rem(w + k, wide)
        to = owner(source)
        s = slot(source)
        here = jnp.where(to == n, s, wide + source)
        remote(piece(source), buf_ref.at[here], send1.at[k], recv1.at[source], "wide", source).wait_recv()

        @pl.when(to != n)
        def _():
            remote(
                buf_ref.at[wide + source], buf_ref.at[s], send2.at[source], recv2.at[s], "narrow", to
            ).start()

    for k in range(1, wide):
        target = lax.rem(w + k, wide)
        remote(piece(target), buf_ref.at[place], send1.at[k], recv1.at[w], "wide", target).wait_send()
    for source in range(wide):
        to = owner(source)

        @pl.when(to != n)
        def _():
            remote(
                buf_ref.at[wide + source], buf_ref.at[source], send2.at[source], recv2.at[source],
                "narrow", to,
            ).wait_send()

    for s in range(wide):
        came = (n * wide + s) % narrow

        @pl.when(came != n)
        def _():
            remote(
                buf_ref.at[s], buf_ref.at[s], send2.at[s], recv2.at[s], "narrow", came
            ).wait_recv()

    @pl.when(mine)
    def _():
        pltpu.make_async_copy(bounce, buf_ref.at[slot(w)], local_sem.at[1]).wait()


def spread(z, wide, narrow):
    rows, order = z.shape
    cols = order // wide
    buf = pl.pallas_call(
        functools.partial(spread_kernel, wide, narrow),
        out_shape=jax.ShapeDtypeStruct((2 * wide, rows, cols), jnp.float32),
        in_specs=[pl.BlockSpec(memory_space=ANY)],
        out_specs=pl.BlockSpec(memory_space=ANY),
        scratch_shapes=[
            VMEM((rows, cols), jnp.float32),
            pltpu.SemaphoreType.DMA((wide,)),
            pltpu.SemaphoreType.DMA((wide,)),
            pltpu.SemaphoreType.DMA((wide,)),
            pltpu.SemaphoreType.DMA((wide,)),
            pltpu.SemaphoreType.DMA((2,)),
        ],
        compiler_params=pltpu.CompilerParams(collective_id=0, has_side_effects=True),
    )(z)
    return buf[:wide].reshape(wide * rows, cols)


def coeffs_kernel(wide, x_ref, t_ref, out_ref, slots, send, recv):
    w = lax.axis_index("wide")
    greet((("wide", wide),))
    for k in range(1, wide):
        target = lax.rem(w + k, wide)
        remote(x_ref, slots.at[w], send.at[k], recv.at[w], "wide", target).start()
    total = x_ref[...]
    for k in range(1, wide):
        source = lax.rem(w + k, wide)
        remote(x_ref, slots.at[source], send.at[k], recv.at[source], "wide", source).wait_recv()
        total = total + slots[source]
    out_ref[...] = lax.dot_general(
        total, t_ref[...], (((1,), (1,)), ((), ())),
        precision=HIGHEST, preferred_element_type=jnp.float32,
    )
    for k in range(1, wide):
        target = lax.rem(w + k, wide)
        remote(x_ref, slots.at[w], send.at[k], recv.at[w], "wide", target).wait_send()


def coeffs_of(products, factor, wide, which):
    return pl.pallas_call(
        functools.partial(coeffs_kernel, wide),
        out_shape=jax.ShapeDtypeStruct(products.shape, jnp.float32),
        in_specs=[pl.BlockSpec(memory_space=VMEM)] * 2,
        out_specs=pl.BlockSpec(memory_space=VMEM),
        scratch_shapes=[
            VMEM((wide,) + products.shape, jnp.float32),
            pltpu.SemaphoreType.DMA((wide,)),
            pltpu.SemaphoreType.DMA((wide,)),
        ],
        compiler_params=pltpu.CompilerParams(collective_id=1 + which, has_side_effects=True),
    )(products, factor)


def chain_kernel(
    wide, corner, lower, diag, out_ref, low_v, diag_v, own, gath, part, land,
    c_send, c_recv, g_send, g_recv, r_send, r_recv, low_sem, diag_sem,
):
    w = lax.axis_index("wide")
    panels, _, count, share = corner.shape
    last = wide - 1
    blocks = lower.shape[0]
    greet((("wide", wide),))

    @pl.when(w == last)
    def _():
        for p in reversed(range(panels)):
            for t in range(last):
                remote(
                    corner.at[p, t], own.at[p], c_send.at[p * wide + t], c_recv.at[p], "wide", t
                ).start()

    def diag_copy(p):
        return pltpu.make_async_copy(diag.at[p], diag_v.at[p], diag_sem.at[p])

    def low_copy(i):
        return pltpu.make_async_copy(lower.at[i], low_v.at[i], low_sem.at[i])

    for p in reversed(range(panels)):
        diag_copy(p).start()
        for q in range(p):
            low_copy(p * (p - 1) // 2 + q).start()

    def gather_copy(p, at, k, target):
        return remote(
            gath.at[p, at], gath.at[p, at], g_send.at[p * wide + k], g_recv.at[p * wide + at],
            "wide", target,
        )

    def reduce_copy(q, at, slot, k, target):
        return remote(
            part.at[q, at], land.at[q, slot], r_send.at[q * wide + k], r_recv.at[q * wide + slot],
            "wide", target,
        )

    def dot(a, b):
        return jnp.dot(a, b, precision=HIGHEST, preferred_element_type=jnp.float32)

    results = [None] * panels
    for p in reversed(range(panels)):

        @pl.when(w == last)
        def _():
            own[p] = corner[p, last]

        @pl.when(w != last)
        def _():
            remote(
                corner.at[p, 0], own.at[p], c_send.at[p * wide], c_recv.at[p], "wide", last
            ).wait_recv()

        remain = own[p]
        if p < panels - 1:
            summed = part[p, w]
            for k in range(1, wide):
                source = lax.rem(w + k, wide)
                reduce_copy(p, source, source, k, source).wait_recv()
                summed = summed + land[p, source]
            remain = remain - summed
        gath[p, w] = remain
        for k in range(1, wide):
            gather_copy(p, w, k, lax.rem(w + k, wide)).start()
        diag_copy(p).wait()

        def rows(source):
            return diag_v[p, pl.ds(pl.multiple_of(source * share, 8), share), :]

        def step(k, acc):
            source = lax.rem(w + k, wide)
            gather_copy(p, source, k, source).wait_recv()
            return acc + dot(gath[p, source], rows(source))

        solved = lax.fori_loop(1, wide, step, dot(remain, rows(w)))
        results[p] = solved
        out_ref[p] = solved
        if p > 0:
            target = p - 1
            total = None
            for j in range(panels - 1, target, -1):
                i = j * (j - 1) // 2 + target
                low_copy(i).wait()
                term = dot(results[j], low_v[i])
                total = term if total is None else total + term
            for t in range(wide):
                part[target, t] = total[:, t * share : (t + 1) * share]
            for k in range(1, wide):
                t = lax.rem(w + k, wide)
                reduce_copy(target, t, w, k, t).start()

    for p in range(panels):
        for k in range(1, wide):
            t = lax.rem(w + k, wide)
            gather_copy(p, w, k, t).wait_send()
            if p < panels - 1:
                reduce_copy(p, t, w, k, t).wait_send()

    @pl.when(w == last)
    def _():
        for p in range(panels):
            for t in range(last):
                remote(
                    corner.at[p, t], own.at[p], c_send.at[p * wide + t], c_recv.at[p], "wide", t
                ).wait_send()


def chain(corner, lower_blocks, diag_inverses, wide):
    panels, _, count, share = corner.shape
    dma = pltpu.SemaphoreType.DMA
    tile = (count, share)
    return pl.pallas_call(
        functools.partial(chain_kernel, wide),
        out_shape=jax.ShapeDtypeStruct((panels,) + tile, jnp.float32),
        in_specs=[
            pl.BlockSpec(memory_space=VMEM),
            pl.BlockSpec(memory_space=ANY),
            pl.BlockSpec(memory_space=ANY),
        ],
        out_specs=pl.BlockSpec(memory_space=VMEM),
        scratch_shapes=[
            VMEM(lower_blocks.shape, jnp.float32),
            VMEM(diag_inverses.shape, jnp.float32),
            VMEM((panels,) + tile, jnp.float32),
            VMEM((panels, wide) + tile, jnp.float32),
            VMEM((panels - 1, wide) + tile, jnp.float32),
            VMEM((panels - 1, wide) + tile, jnp.float32),
            dma((panels * wide,)),
            dma((panels,)),
            dma((panels * wide,)),
            dma((panels * wide,)),
            dma(((panels - 1) * wide,)),
            dma(((panels - 1) * wide,)),
            dma((lower_blocks.shape[0],)),
            dma((panels,)),
        ],
        compiler_params=pltpu.CompilerParams(
            collective_id=3, has_side_effects=True, vmem_limit_bytes=48 * 1024 * 1024
        ),
    )(corner, lower_blocks, diag_inverses)


def body(tridiag_vectors, reflectors, triangles, lower_blocks, diag_inverses):
    wide = lax.axis_size("wide")
    narrow = lax.axis_size("narrow")
    current = spread(tridiag_vectors, wide, narrow)
    for which in (1, 0):
        products = jnp.dot(current, reflectors[which], precision=HIGHEST)
        coeffs = coeffs_of(products, triangles[which], wide, which)
        current = current - jnp.dot(coeffs, reflectors[which].T, precision=HIGHEST)
    panels, panel_rows, share = diag_inverses.shape
    tail = current[:, current.shape[1] - panels * panel_rows :]
    corner = tail.reshape(tail.shape[0], panels, wide, share).transpose(1, 2, 0, 3)
    solved = chain(corner, lower_blocks, diag_inverses, wide)
    return current, solved.transpose(1, 0, 2)


def solution(mesh):
    placed = (
        P(("wide", "narrow"), None),
        P(None, "wide", None),
        P(),
        P(None, "wide", None),
        P(None, None, "wide"),
    )
    return jax.shard_map(
        body,
        mesh=mesh,
        in_specs=placed,
        out_specs=(P("narrow", "wide"), P("narrow", None, "wide")),
        check_vma=False,
    )
```

```python
import functools

import jax
import jax.numpy as jnp
from jax import lax
from jax.experimental import pallas as pl
from jax.experimental.pallas import tpu as pltpu
from jax.sharding import PartitionSpec as P

HIGHEST = lax.Precision.HIGHEST
MESH = pl.DeviceIdType.MESH
ANY = pl.ANY
VMEM = pltpu.VMEM


def greet(axes):
    barrier = pltpu.get_barrier_semaphore()
    total = 0
    for axis, size in axes:
        here = lax.axis_index(axis)
        for k in range(1, size):
            pl.semaphore_signal(
                barrier, inc=1, device_id={axis: lax.rem(here + k, size)}, device_id_type=MESH
            )
        total += size - 1
    pl.semaphore_wait(barrier, total)


def remote(src, dst, send, recv, axis, target):
    return pltpu.make_async_remote_copy(
        src_ref=src, dst_ref=dst, send_sem=send, recv_sem=recv,
        device_id={axis: target}, device_id_type=MESH,
    )


def spread_kernel(
    wide, narrow, z_ref, turned_ref, buf_ref, diag_ref, bounce, raw, turned,
    send1, recv1, send2, recv2, local_sem, raw_sem, turned_sem,
):
    w = lax.axis_index("wide")
    n = lax.axis_index("narrow")
    cols = buf_ref.shape[2]

    def piece(target):
        return z_ref.at[:, pl.ds(pl.multiple_of(target * cols, 128), cols)]

    def owner(source):
        return (source * narrow + n) // wide

    def slot(source):
        return (source * narrow + n) % wide

    panels = turned_ref.shape[0]

    def load(p):
        return pltpu.make_async_copy(turned_ref.at[p], raw.at[p], raw_sem.at[p])

    def store(p):
        return pltpu.make_async_copy(turned.at[p], diag_ref.at[p], turned_sem.at[p])

    def turn(p):
        load(p).wait()
        turned[p] = raw[p].T
        store(p).start()

    greet((("wide", wide), ("narrow", narrow)))
    place = jnp.where(owner(w) == n, slot(w), wide + w)
    for k in range(1, wide):
        target = lax.rem(w + k, wide)
        remote(piece(target), buf_ref.at[place], send1.at[k], recv1.at[w], "wide", target).start()

    for p in range(panels):
        load(p).start()
    mine = owner(w) == n

    @pl.when(mine)
    def _():
        first = pltpu.make_async_copy(piece(w), bounce, local_sem.at[0])
        first.start()
        first.wait()
        pltpu.make_async_copy(bounce, buf_ref.at[slot(w)], local_sem.at[1]).start()

    @pl.when(jnp.logical_not(mine))
    def _():
        s = slot(w)
        remote(piece(w), buf_ref.at[s], send2.at[w], recv2.at[s], "narrow", owner(w)).start()

    for k in range(1, wide):
        if k <= panels:
            turn(k - 1)
        source = lax.rem(w + wide - k, wide)
        to = owner(source)
        s = slot(source)
        here = jnp.where(to == n, s, wide + source)
        remote(piece(source), buf_ref.at[here], send1.at[k], recv1.at[source], "wide", source).wait_recv()

        @pl.when(to != n)
        def _():
            remote(
                buf_ref.at[wide + source], buf_ref.at[s], send2.at[source], recv2.at[s], "narrow", to
            ).start()

    for p in range(wide - 1, panels):
        turn(p)
    for k in range(1, wide):
        target = lax.rem(w + k, wide)
        remote(piece(target), buf_ref.at[place], send1.at[k], recv1.at[w], "wide", target).wait_send()
    for p in range(panels):
        store(p).wait()
    for source in range(wide):
        to = owner(source)

        @pl.when(to != n)
        def _():
            remote(
                buf_ref.at[wide + source], buf_ref.at[source], send2.at[source], recv2.at[source],
                "narrow", to,
            ).wait_send()

    for s in range(wide):
        came = (n * wide + s) % narrow

        @pl.when(came != n)
        def _():
            remote(
                buf_ref.at[s], buf_ref.at[s], send2.at[s], recv2.at[s], "narrow", came
            ).wait_recv()

    @pl.when(mine)
    def _():
        pltpu.make_async_copy(bounce, buf_ref.at[slot(w)], local_sem.at[1]).wait()


def spread(z, turned, wide, narrow):
    rows, order = z.shape
    cols = order // wide
    panels, share, panel_rows = turned.shape
    diag_shape = (panels, panel_rows, share)
    buf, diag = pl.pallas_call(
        functools.partial(spread_kernel, wide, narrow),
        out_shape=(
            jax.ShapeDtypeStruct((2 * wide, rows, cols), jnp.float32),
            jax.ShapeDtypeStruct(diag_shape, jnp.float32),
        ),
        in_specs=[pl.BlockSpec(memory_space=ANY)] * 2,
        out_specs=[pl.BlockSpec(memory_space=ANY)] * 2,
        scratch_shapes=[
            VMEM((rows, cols), jnp.float32),
            VMEM(turned.shape, jnp.float32),
            VMEM(diag_shape, jnp.float32),
            pltpu.SemaphoreType.DMA((wide,)),
            pltpu.SemaphoreType.DMA((wide,)),
            pltpu.SemaphoreType.DMA((wide,)),
            pltpu.SemaphoreType.DMA((wide,)),
            pltpu.SemaphoreType.DMA((2,)),
            pltpu.SemaphoreType.DMA((panels,)),
            pltpu.SemaphoreType.DMA((panels,)),
        ],
        compiler_params=pltpu.CompilerParams(collective_id=0, has_side_effects=True),
    )(z, turned)
    return buf[:wide].reshape(wide * rows, cols), diag


def coeffs_kernel(wide, x_ref, t_ref, out_ref, slots, send, recv):
    w = lax.axis_index("wide")
    greet((("wide", wide),))
    for k in range(1, wide):
        target = lax.rem(w + k, wide)
        remote(x_ref, slots.at[w], send.at[k], recv.at[w], "wide", target).start()
    total = x_ref[...]
    for k in range(1, wide):
        source = lax.rem(w + k, wide)
        remote(x_ref, slots.at[source], send.at[k], recv.at[source], "wide", source).wait_recv()
        total = total + slots[source]
    out_ref[...] = lax.dot_general(
        t_ref[...], total, (((1,), (1,)), ((), ())),
        precision=HIGHEST, preferred_element_type=jnp.float32,
    )
    for k in range(1, wide):
        target = lax.rem(w + k, wide)
        remote(x_ref, slots.at[w], send.at[k], recv.at[w], "wide", target).wait_send()


def coeffs_of(products, factor, wide, which):
    return pl.pallas_call(
        functools.partial(coeffs_kernel, wide),
        out_shape=jax.ShapeDtypeStruct((factor.shape[0], products.shape[0]), jnp.float32),
        in_specs=[pl.BlockSpec(memory_space=VMEM)] * 2,
        out_specs=pl.BlockSpec(memory_space=VMEM),
        scratch_shapes=[
            VMEM((wide,) + products.shape, jnp.float32),
            pltpu.SemaphoreType.DMA((wide,)),
            pltpu.SemaphoreType.DMA((wide,)),
        ],
        compiler_params=pltpu.CompilerParams(collective_id=1 + which, has_side_effects=True),
    )(products, factor)


def update_kernel(z_ref, r_ref, c_ref, out_ref):
    change = jnp.dot(
        r_ref[0], c_ref[...], precision=HIGHEST, preferred_element_type=jnp.float32
    )
    out_ref[...] = z_ref[...] - change.T


def update(current, reflectors, coeffs, which):
    count, cols = current.shape
    depth = reflectors.shape[2]
    chunk = 1024 if cols % 1024 == 0 else 128
    return pl.pallas_call(
        update_kernel,
        grid=(cols // chunk,),
        out_shape=jax.ShapeDtypeStruct(current.shape, jnp.float32),
        in_specs=[
            pl.BlockSpec((count, chunk), lambda i: (0, i)),
            pl.BlockSpec((1, chunk, depth), lambda i: (which, i, 0)),
            pl.BlockSpec((depth, count), lambda i: (0, 0)),
        ],
        out_specs=pl.BlockSpec((count, chunk), lambda i: (0, i)),
        cost_estimate=pl.CostEstimate(
            flops=2 * count * cols * depth,
            bytes_accessed=4 * cols * (depth + 2 * count),
            transcendentals=0,
        ),
    )(current, reflectors, coeffs)


def chain_kernel(
    wide, corner, lower, diag, out_ref, low_v, diag_v, own, gath, part, land,
    c_send, c_recv, g_send, g_recv, r_send, r_recv, low_sem, diag_sem,
):
    w = lax.axis_index("wide")
    panels, _, count, share = corner.shape
    last = wide - 1
    blocks = lower.shape[0]
    greet((("wide", wide),))

    @pl.when(w == last)
    def _():
        for p in reversed(range(panels)):
            for t in range(last):
                remote(
                    corner.at[p, t], own.at[p], c_send.at[p * wide + t], c_recv.at[p], "wide", t
                ).start()

    def diag_copy(p):
        return pltpu.make_async_copy(diag.at[p], diag_v.at[p], diag_sem.at[p])

    def low_copy(i):
        return pltpu.make_async_copy(lower.at[i], low_v.at[i], low_sem.at[i])

    for p in reversed(range(panels)):
        diag_copy(p).start()
        for q in range(p):
            low_copy(p * (p - 1) // 2 + q).start()

    def gather_copy(p, at, k, target):
        return remote(
            gath.at[p, at], gath.at[p, at], g_send.at[p * wide + k], g_recv.at[p * wide + at],
            "wide", target,
        )

    def reduce_copy(q, at, slot, k, target):
        return remote(
            part.at[q, at], land.at[q, slot], r_send.at[q * wide + k], r_recv.at[q * wide + slot],
            "wide", target,
        )

    def dot(a, b):
        return jnp.dot(a, b, precision=HIGHEST, preferred_element_type=jnp.float32)

    results = [None] * panels
    for p in reversed(range(panels)):

        @pl.when(w == last)
        def _():
            own[p] = corner[p, last]

        @pl.when(w != last)
        def _():
            remote(
                corner.at[p, 0], own.at[p], c_send.at[p * wide], c_recv.at[p], "wide", last
            ).wait_recv()

        remain = own[p]
        if p < panels - 1:
            summed = part[p, w]
            for k in range(1, wide):
                source = lax.rem(w + k, wide)
                reduce_copy(p, source, source, k, source).wait_recv()
                summed = summed + land[p, source]
            remain = remain - summed
        gath[p, w] = remain
        for k in range(1, wide):
            gather_copy(p, w, k, lax.rem(w + k, wide)).start()
        diag_copy(p).wait()

        def rows(source):
            return diag_v[p, pl.ds(pl.multiple_of(source * share, 8), share), :]

        def step(k, acc):
            source = lax.rem(w + k, wide)
            gather_copy(p, source, k, source).wait_recv()
            return acc + dot(gath[p, source], rows(source))

        solved = lax.fori_loop(1, wide, step, dot(remain, rows(w)))
        results[p] = solved
        out_ref[p] = solved
        if p > 0:
            target = p - 1
            total = None
            for j in range(panels - 1, target, -1):
                i = j * (j - 1) // 2 + target
                low_copy(i).wait()
                term = dot(results[j], low_v[i])
                total = term if total is None else total + term
            for t in range(wide):
                part[target, t] = total[:, t * share : (t + 1) * share]
            for k in range(1, wide):
                t = lax.rem(w + k, wide)
                reduce_copy(target, t, w, k, t).start()

    for p in range(panels):
        for k in range(1, wide):
            t = lax.rem(w + k, wide)
            gather_copy(p, w, k, t).wait_send()
            if p < panels - 1:
                reduce_copy(p, t, w, k, t).wait_send()

    @pl.when(w == last)
    def _():
        for p in range(panels):
            for t in range(last):
                remote(
                    corner.at[p, t], own.at[p], c_send.at[p * wide + t], c_recv.at[p], "wide", t
                ).wait_send()


def chain(corner, lower_blocks, diag_inverses, wide):
    panels, _, count, share = corner.shape
    dma = pltpu.SemaphoreType.DMA
    tile = (count, share)
    return pl.pallas_call(
        functools.partial(chain_kernel, wide),
        out_shape=jax.ShapeDtypeStruct((panels,) + tile, jnp.float32),
        in_specs=[
            pl.BlockSpec(memory_space=VMEM),
            pl.BlockSpec(memory_space=ANY),
            pl.BlockSpec(memory_space=ANY),
        ],
        out_specs=pl.BlockSpec(memory_space=VMEM),
        scratch_shapes=[
            VMEM(lower_blocks.shape, jnp.float32),
            VMEM(diag_inverses.shape, jnp.float32),
            VMEM((panels,) + tile, jnp.float32),
            VMEM((panels, wide) + tile, jnp.float32),
            VMEM((panels - 1, wide) + tile, jnp.float32),
            VMEM((panels - 1, wide) + tile, jnp.float32),
            dma((panels * wide,)),
            dma((panels,)),
            dma((panels * wide,)),
            dma((panels * wide,)),
            dma(((panels - 1) * wide,)),
            dma(((panels - 1) * wide,)),
            dma((lower_blocks.shape[0],)),
            dma((panels,)),
        ],
        compiler_params=pltpu.CompilerParams(
            collective_id=3, has_side_effects=True, vmem_limit_bytes=48 * 1024 * 1024
        ),
    )(corner, lower_blocks, diag_inverses)


def body(tridiag_vectors, reflectors, triangles, lower_blocks, diag_inverses):
    wide = lax.axis_size("wide")
    narrow = lax.axis_size("narrow")
    current, diag = spread(
        tridiag_vectors, diag_inverses.transpose(0, 2, 1), wide, narrow
    )
    for which in (1, 0):
        products = jnp.dot(current, reflectors[which], precision=HIGHEST)
        coeffs = coeffs_of(products, triangles[which], wide, which)
        current = update(current, reflectors, coeffs, which)
    panels, panel_rows, share = diag_inverses.shape
    tail = current[:, current.shape[1] - panels * panel_rows :]
    corner = tail.reshape(tail.shape[0], panels, wide, share).transpose(1, 2, 0, 3)
    solved = chain(corner, lower_blocks, diag, wide)
    return current, solved.transpose(1, 0, 2)


def solution(mesh):
    placed = (
        P(("wide", "narrow"), None),
        P(None, "wide", None),
        P(),
        P(None, "wide", None),
        P(None, None, "wide"),
    )
    return jax.shard_map(
        body,
        mesh=mesh,
        in_specs=placed,
        out_specs=(P("narrow", "wide"), P("narrow", None, "wide")),
        check_vma=False,
    )
```
